128 devices in a mesh: row: 8 (over z, core), col: 16 (over y, x).
Axes of the slice: x: 4, y: 4, z: 4, core: 2. Of those that a mesh axis runs over, the one named last changes fastest.
Arguments:
- fine_residual: bfloat16 [16, 2097152], P(None, ('row', 'col')), may hold values from -6 to 6
- tiles_one: bfloat16 [65536, 128, 128], P(('row', 'col')), may hold values from -0.125 to 0.125
- pointers_one: int32 [32896], P(('row', 'col')), may hold values from 0 to 512, as said below
- columns_one: int32 [65536], P(('row', 'col')), may hold values from 0 to 2047, as said below
- points_one: int32 [524288], P(('col', 'row')), may hold values from 0 to 16383, as said below
- tiles_two: bfloat16 [32768, 128, 128], P(('row', 'col')), may hold values from -0.09375 to 0.09375
- pointers_two: int32 [16512], P(('row', 'col')), may hold values from 0 to 256, as said below
- columns_two: int32 [32768], P(('row', 'col')), may hold values from 0 to 255
- points_two: int32 [131072], P(('row', 'col')), may hold values from 0 to 4095, as said below
- tiles_three: bfloat16 [4096, 128, 128], P(('row', 'col')), may hold values from -0.125 to 0.125
- pointers_three: int32 [2176], P(('row', 'col')), may hold values from 0 to 32, as said below
- columns_three: int32 [4096], P(('row', 'col')), may hold values from 0 to 127
- points_three: int32 [32768], P(('col', 'row')), may hold values from 0 to 1023, as said below
Outputs:
- coarse_one: bfloat16 [16, 524288], P(None, ('col', 'row'))
- coarse_two: bfloat16 [16, 131072], P(None, ('row', 'col'))
- coarse_three: bfloat16 [16, 32768], P(None, ('col', 'row'))
The draws below stay inside these ranges and needn't reach their ends.
Inputs may be any that keep to these rules, and one draw needn't show every extreme that they name: `pointers_one`: each tile set's 256 + 1 pointers start at 0 and never fall; the last is that set's live slot count, at most 512; some set has 512 live slots. `pointers_two`: each tile set's 128 + 1 pointers start at 0 and never fall; the last is that set's live slot count, at most 256; some set has 256 live slots. `pointers_three`: each tile set's 16 + 1 pointers start at 0 and never fall; the last is that set's live slot count, at most 32; some set has 32 live slots. `columns_one`: among the live slots of one tile set, at most 32 name block columns with the same quotient by 128; some set reaches 32. `points_one`: values are distinct within each aligned run of 4096 entries. `points_two`: values are distinct within each aligned run of 1024 entries. `points_three`: values are distinct within each aligned run of 256 entries.
All inputs are finite; a program needn't handle non-finite values.
Results may differ from the reference program's by a relative error of at most 0.0057.
Values may be sent and summed in bfloat16 or wider, within the bound.
A program may use at most 128 MiB of HBM per device.

```python
import jax
import jax.numpy as jnp
from jax import lax

TILE_EDGE = 128
VECTORS = 16
PIECE_ROWS = 16384
FINE_ROWS = 2097152
COARSE_ONE = 524288
COARSE_TWO = 131072
COARSE_THREE = 32768
BLOCKS_ONE = 256
BLOCKS_TWO = 128
BLOCKS_THREE = 16
SLOTS_ONE = 512
SLOTS_TWO = 256
SLOTS_THREE = 32
FINE_BLOCKS_TWO = 256
FINE_BLOCKS_THREE = 128
PEER_SLOTS = 32
N_ROW = 8
N_COL = 16
DEVICES = 128


def live_counts(level_key, slot_count):
    shifts = jax.random.randint(jax.random.fold_in(level_key, 11), (DEVICES,), 0, 5)
    forced = jax.random.randint(jax.random.fold_in(level_key, 12), (), 0, DEVICES)
    shifts = jnp.where(jnp.arange(DEVICES) == forced, 0, shifts)
    full_slots = jnp.full((DEVICES,), slot_count, jnp.int32)
    return jnp.maximum(jnp.right_shift(full_slots, shifts.astype(jnp.int32)), 1).astype(jnp.int32)


def pointer_table(level_key, slot_count, block_count):
    counts = live_counts(level_key, slot_count)
    block_draw = jax.random.randint(jax.random.fold_in(level_key, 13), (DEVICES, slot_count), 0, block_count)
    positions = jnp.arange(slot_count, dtype=jnp.int32)
    block_draw = jnp.where(positions[None, :] < counts[:, None], block_draw, block_count)
    ordered = jnp.sort(block_draw, axis=1)
    bounds = jnp.arange(block_count + 1, dtype=jnp.int32)
    table = jnp.sum((ordered[:, None, :] < bounds[None, :, None]).astype(jnp.int32), axis=2)
    return table.reshape(-1).astype(jnp.int32)


def point_table(level_key, piece_in, piece_out):
    keys = jax.random.split(level_key, DEVICES)
    chosen = jax.vmap(lambda single: jax.random.permutation(single, piece_in)[:piece_out])(keys)
    return chosen.reshape(-1).astype(jnp.int32)


def draw_pointers_one(key, part):
    return pointer_table(jax.random.fold_in(key, 1), SLOTS_ONE, BLOCKS_ONE)


def draw_pointers_two(key, part):
    return pointer_table(jax.random.fold_in(key, 2), SLOTS_TWO, BLOCKS_TWO)


def draw_pointers_three(key, part):
    return pointer_table(jax.random.fold_in(key, 3), SLOTS_THREE, BLOCKS_THREE)


def draw_columns_one(key, part):
    level_key = jax.random.fold_in(key, 1)
    counts = live_counts(level_key, SLOTS_ONE)
    blocks_peer = PIECE_ROWS // TILE_EDGE
    positions = jnp.arange(SLOTS_ONE, dtype=jnp.int32)
    is_live = positions[None, :] < counts[:, None]
    scores = jax.random.randint(jax.random.fold_in(key, 21), (DEVICES, SLOTS_ONE), 0, 1 << 20) * SLOTS_ONE + positions[None, :]
    scores = jnp.where(is_live, scores, scores + (1 << 30))
    rank_order = jnp.argsort(scores, axis=1)
    hot_rank = jnp.argsort(rank_order, axis=1)
    hot_take = jnp.minimum(counts, PEER_SLOTS)
    is_hot = hot_rank < hot_take[:, None]
    hot_peer = jax.random.randint(jax.random.fold_in(key, 22), (DEVICES,), 0, N_COL)
    base_list = jnp.arange((N_COL - 1) * PEER_SLOTS, dtype=jnp.int32) % (N_COL - 1)
    other_keys = jax.random.split(jax.random.fold_in(key, 23), DEVICES)
    others = jax.vmap(lambda single: jax.random.permutation(single, base_list))(other_keys)
    other_rank = jnp.cumsum(1 - is_hot.astype(jnp.int32), axis=1) - 1
    other_rank = jnp.clip(other_rank, 0, (N_COL - 1) * PEER_SLOTS - 1)
    other_choice = jnp.take_along_axis(others, other_rank, axis=1)
    owner_peer = jnp.where(is_hot, hot_peer[:, None], (hot_peer[:, None] + 1 + other_choice) % N_COL)
    offsets = jax.random.randint(jax.random.fold_in(key, 24), (DEVICES, SLOTS_ONE), 0, blocks_peer)
    return (owner_peer * blocks_peer + offsets).reshape(-1).astype(jnp.int32)


def draw_points_one(key, part):
    return point_table(jax.random.fold_in(key, 31), PIECE_ROWS, PIECE_ROWS // 4)


def draw_points_two(key, part):
    return point_table(jax.random.fold_in(key, 32), PIECE_ROWS // 4, PIECE_ROWS // 16)


def draw_points_three(key, part):
    return point_table(jax.random.fold_in(key, 33), PIECE_ROWS // 16, PIECE_ROWS // 64)


def plant(result, own_key, least, largest):
    dims = result.shape
    spot = [jax.random.randint(jax.random.fold_in(own_key, axis), (), 0, dims[axis]) for axis in range(len(dims))]
    result = result.at[tuple(spot)].set(least)
    longest = dims.index(max(dims))
    spot[longest] = (spot[longest] + 1) % dims[longest]
    return result.at[tuple(spot)].set(largest)


def block_scale(rng, extent, cuts, low, high):
    def one(position, blocks):
        draws = jax.random.uniform(jax.random.fold_in(jax.random.fold_in(rng, 6), position), (blocks,), jnp.float32, low / len(cuts), high / len(cuts))
        return jnp.repeat(jnp.exp(draws), extent[position] // blocks).reshape((-1,) + (1,) * (len(extent) - position - 1))

    level = one(*cuts[0])
    for cut in cuts[1:]:
        level = level * one(*cut)
    return level


def gaussian(rng, shape, deviation, most, pieces=(), kind=jnp.bfloat16):
    array = jax.random.normal(rng, shape, jnp.float32) * deviation
    if len(pieces) > 0:
        array = block_scale(rng, shape, pieces, -0.22, 0.18) * array
    return jnp.clip(array, min=-most, max=most).astype(kind)


def setup_inputs(seed: int = 0) -> dict:
    arg_keys = jax.random.split(jax.random.key(seed), 14)
    return {
        "fine_residual": gaussian(arg_keys[0], (VECTORS, FINE_ROWS), 1.0, 6.0, ((1, 128),)),
        "tiles_one": gaussian(arg_keys[1], (DEVICES * SLOTS_ONE, TILE_EDGE, TILE_EDGE), (2 * TILE_EDGE * N_ROW) ** -0.5, 0.125, ((0, 128),)),
        "pointers_one": draw_pointers_one(jax.random.fold_in(arg_keys[13], 71), 0),
        "columns_one": draw_columns_one(jax.random.fold_in(arg_keys[13], 71), 0),
        "points_one": draw_points_one(jax.random.fold_in(arg_keys[13], 71), 0),
        "tiles_two": gaussian(arg_keys[5], (DEVICES * SLOTS_TWO, TILE_EDGE, TILE_EDGE), (2 * TILE_EDGE * N_COL) ** -0.5, 0.09375, ((0, 128),)),
        "pointers_two": draw_pointers_two(jax.random.fold_in(arg_keys[13], 71), 0),
        "columns_two": plant(jax.random.randint(arg_keys[7], (DEVICES * SLOTS_TWO,), 0, FINE_BLOCKS_TWO), jax.random.fold_in(arg_keys[7], 1), 0, FINE_BLOCKS_TWO - 1).astype(jnp.int32),
        "points_two": draw_points_two(jax.random.fold_in(arg_keys[13], 71), 0),
        "tiles_three": gaussian(arg_keys[9], (DEVICES * SLOTS_THREE, TILE_EDGE, TILE_EDGE), (2 * TILE_EDGE * N_ROW) ** -0.5, 0.125, ((0, 128),)),
        "pointers_three": draw_pointers_three(jax.random.fold_in(arg_keys[13], 71), 0),
        "columns_three": plant(jax.random.randint(arg_keys[11], (DEVICES * SLOTS_THREE,), 0, FINE_BLOCKS_THREE), jax.random.fold_in(arg_keys[11], 1), 0, FINE_BLOCKS_THREE - 1).astype(jnp.int32),
        "points_three": draw_points_three(jax.random.fold_in(arg_keys[13], 71), 0),
    }


def level_tiles(vector, tiles, columns, pointers, slot_count, block_count, fine_size, coarse_size, coarse_total, even_level):
    tile_edge = tiles.shape[1]
    vector_count = vector.shape[0]
    positions = jnp.arange(slot_count, dtype=jnp.int32)

    def one_device(running, device):
        if even_level:
            fine_index = device // N_COL
            coarse_index = device % N_COL
        else:
            fine_index = device % N_COL
            coarse_index = device // N_COL
        my_tiles = lax.dynamic_slice_in_dim(tiles, (device * slot_count).astype(jnp.int32), slot_count, 0).astype(jnp.float32)
        my_columns = lax.dynamic_slice_in_dim(columns, (device * slot_count).astype(jnp.int32), slot_count, 0)
        my_pointers = lax.dynamic_slice_in_dim(pointers, (device * (block_count + 1)).astype(jnp.int32), block_count + 1, 0)
        is_live = positions < my_pointers[block_count]
        finished = jnp.sum((my_pointers[1:][None, :] <= positions[:, None]).astype(jnp.int32), axis=1)
        segment = jnp.where(is_live, finished, block_count).astype(jnp.int32)
        fine_group = lax.dynamic_slice_in_dim(vector, (fine_index * fine_size).astype(jnp.int32), fine_size, 1).astype(jnp.float32)
        blocks = fine_group.reshape(vector_count, fine_size // tile_edge, tile_edge)
        picked = jnp.take(blocks, my_columns, axis=1)
        products = jnp.einsum("sij,vsj->svi", my_tiles, picked, precision=lax.Precision.HIGHEST)
        summed = jax.ops.segment_sum(products, segment, num_segments=block_count + 1)[:block_count]
        part_sum = jnp.transpose(summed, (1, 0, 2)).reshape(vector_count, coarse_size)
        offset = (coarse_index * coarse_size).astype(jnp.int32)
        current = lax.dynamic_slice_in_dim(running, offset, coarse_size, 1)
        return lax.dynamic_update_slice_in_dim(running, current + part_sum, offset, 1), None

    initial = jnp.zeros((vector_count, coarse_total), jnp.float32)
    running, unused = lax.scan(one_device, initial, jnp.arange(DEVICES, dtype=jnp.int32))
    return running


def point_rows(points, piece_in, piece_out, even_level):
    piece_index = jnp.arange(points.shape[0], dtype=jnp.int32) // piece_out
    if even_level:
        grid_row = piece_index % N_ROW
        grid_col = piece_index // N_ROW
        source = grid_row * N_COL + grid_col
    else:
        grid_row = piece_index // N_COL
        grid_col = piece_index % N_COL
        source = grid_col * N_ROW + grid_row
    return (source * piece_in + points).astype(jnp.int32)


def restrict(vector, tiles, columns, pointers, points, slot_count, block_count, fine_size, coarse_size, coarse_total, piece_in, even_level):
    running = level_tiles(vector, tiles, columns, pointers, slot_count, block_count, fine_size, coarse_size, coarse_total, even_level)
    fine_point = point_rows(points, piece_in, coarse_total // DEVICES, even_level)
    injected = jnp.take(vector, fine_point, axis=1).astype(jnp.float32)
    return (running + injected).astype(jnp.bfloat16)


def reference(fine_residual, tiles_one, pointers_one, columns_one, points_one, tiles_two, pointers_two, columns_two, points_two, tiles_three, pointers_three, columns_three, points_three):
    coarse_one = restrict(fine_residual, tiles_one, columns_one, pointers_one, points_one, SLOTS_ONE, BLOCKS_ONE, FINE_ROWS // N_ROW, COARSE_ONE // N_COL, COARSE_ONE, PIECE_ROWS, True)
    coarse_two = restrict(coarse_one, tiles_two, columns_two, pointers_two, points_two, SLOTS_TWO, BLOCKS_TWO, COARSE_ONE // N_COL, COARSE_TWO // N_ROW, COARSE_TWO, PIECE_ROWS // 4, False)
    coarse_three = restrict(coarse_two, tiles_three, columns_three, pointers_three, points_three, SLOTS_THREE, BLOCKS_THREE, COARSE_TWO // N_ROW, COARSE_THREE // N_COL, COARSE_THREE, PIECE_ROWS // 16, True)
    return (coarse_one, coarse_two, coarse_three)
```

```python
import jax
import jax.numpy as jnp
from jax import lax
from jax.experimental import pallas as pl
from jax.experimental.pallas import tpu as pltpu
from jax.sharding import PartitionSpec as P

MESH = pl.DeviceIdType.MESH
F32 = jnp.float32
BF16 = jnp.bfloat16
I32 = jnp.int32
E = 128
V = 16
ORDER = (
    (1, 1), (3, 3), (0, 2), (1, 3), (3, 1), (2, 0), (1, 2), (3, 2),
    (2, 1), (2, 3), (0, 1), (0, 3), (1, 0), (3, 0), (2, 2),
)
NT = (((1,), (1,)), ((), ()))


def inject(load, n_src, points, first, group, store):
    low, high = [], []
    for i in range(group):
        row = jnp.broadcast_to(points[pl.ds(first + i, 1), :], (V, E))
        low.append(row & (E - 1))
        high.append(row >> 7)

    def source(j, held):
        block = load(j).astype(F32)
        return tuple(
            jnp.where(
                high[i] == j,
                jnp.take_along_axis(block, low[i], axis=1, mode="promise_in_bounds"),
                held[i],
            )
            for i in range(group)
        )

    zero = jnp.zeros((V, E), F32)
    held = lax.fori_loop(0, n_src, source, (zero,) * group, unroll=8)
    for i in range(group):
        store(i, held[i])


def plan(ptr1, cols1, ask, slot, tgt):
    n1 = cols1.shape[1]
    live = ptr1[ptr1.shape[0] - 1]
    names = cols1[...]
    lanes = lax.broadcasted_iota(I32, (1, n1), 1)
    owner = names >> 7
    hit = jnp.where(
        (lax.broadcasted_iota(I32, (16, n1), 0) == owner) & (lanes < live), 1.0, 0.0
    ).astype(F32)
    before = jnp.where(
        lax.broadcasted_iota(I32, (n1, n1), 0) < lax.broadcasted_iota(I32, (n1, n1), 1), 1.0, 0.0
    ).astype(BF16)
    count = jnp.dot(hit.astype(BF16), before, preferred_element_type=F32)
    rank = jnp.sum(hit * count, axis=0, keepdims=True)
    tgt[...] = jnp.where(lanes < live, owner * 32 + rank.astype(I32), 0)
    place = jnp.where(
        lax.broadcasted_iota(I32, (E, n1), 0).astype(F32) == rank, 1.0, 0.0
    ).astype(BF16)
    listed = jnp.concatenate(
        [
            hit * (names & (E - 1)).astype(F32),
            hit * (lanes >> 8).astype(F32),
            hit * (lanes & 255).astype(F32),
        ],
        axis=0,
    ).astype(BF16)
    table = lax.dot_general(listed, place, NT, preferred_element_type=F32).astype(I32)
    for p in range(16):
        ask[p] = table[p : p + 1]
        slot[p] = table[16 + p : 17 + p] * 256 + table[32 + p : 33 + p]


def kernel(
    ask, pts1, pts2, pts3, s_tgt, s_slot, ptr1, cols2, ptr2, cols3, ptr3,
    fine_hbm, t1_hbm, t2_hbm, t3_hbm,
    out1_hbm, out2_hbm, out3_hbm,
    fine, blocks, t1, t2, t3,
    asked, s_asked,
    snd, got, prod, run,
    d_snd, d_got, own1, z_snd, z_got, inj1, g1,
    c_snd, c_got, own2, inj2, g2,
    r_snd, r_got, out1, out2, out3,
    ld_sem, t_sem, ix_sem,
    ask_s, ask_r, rep_s, rep_r, d_s, d_r, z_s, z_r, a_s, a_r,
    p_s, p_r, q_s, q_r, m_s, m_r, o_sem,
):
    row = lax.axis_index("row")
    col = lax.axis_index("col")
    z, core = row // 2, lax.rem(row, 2)
    y, x = col // 4, lax.rem(col, 4)
    other = 1 - core

    def at(dx, dy):
        return lax.rem(y + dy, 4) * 4 + lax.rem(x + dx, 4)

    def remote(src, dst, send, recv, **device):
        return pltpu.make_async_remote_copy(
            src_ref=src, dst_ref=dst, send_sem=send, recv_sem=recv,
            device_id=device, device_id_type=MESH,
        )

    load_fine = pltpu.make_async_copy(fine_hbm, fine, ld_sem.at[0])
    load_fine.start()
    load_t1 = pltpu.make_async_copy(t1_hbm, t1, t_sem.at[0])
    load_t1.start()
    load_t2 = pltpu.make_async_copy(t2_hbm, t2, t_sem.at[1])
    load_t3 = pltpu.make_async_copy(t3_hbm, t3, t_sem.at[2])

    barrier = pltpu.get_barrier_semaphore()
    for d in range(1, 16):
        pl.semaphore_signal(barrier, inc=1, device_id={"col": lax.rem(col + d, 16)}, device_id_type=MESH)
    for d in range(1, 8):
        pl.semaphore_signal(barrier, inc=1, device_id={"row": lax.rem(row + d, 8)}, device_id_type=MESH)

    pl.semaphore_wait(barrier, 22)

    asks = []
    for dx, dy in ORDER:
        peer = at(dx, dy)
        copy = remote(ask.at[peer], asked.at[col], ask_s.at[peer], ask_r.at[col], col=peer)
        copy.start()
        asks.append(copy)
    asked[col] = ask[col]
    load_fine.wait()

    def cut(j, carry):
        blocks[j] = fine[:, pl.ds(pl.multiple_of(j * E, E), E)]
        return carry

    lax.fori_loop(0, 128, cut, 0, unroll=8)
    for dx, dy in ORDER:
        peer = at(dx, dy)
        remote(ask.at[peer], asked.at[peer], ask_s.at[peer], ask_r.at[peer], col=peer).wait_recv()
    copy_asked = pltpu.make_async_copy(asked, s_asked, ix_sem.at[0])
    copy_asked.start()
    copy_asked.wait()

    replies = []

    def pick(peer, k):
        return blocks[s_asked[peer, 0, k]]

    for half in range(2):
        for dx, dy in ORDER:
            peer = at(dx, dy)

            def fill(k, carry, peer=peer):
                snd[peer, k] = pick(peer, k)
                return carry

            lax.fori_loop(half * 16, half * 16 + 16, fill, 0, unroll=8)
            part = pl.ds(half * 16, 16)
            copy = remote(
                snd.at[peer, part], got.at[col, part], rep_s.at[peer, half], rep_r.at[col, half], col=peer
            )
            copy.start()
            replies.append(copy)

    def fill_own(k, carry):
        got[col, k] = pick(col, k)
        return carry

    lax.fori_loop(0, 32, fill_own, 0, unroll=8)
    load_t2.start()
    load_t3.start()

    def inject_one(g, carry):
        def store(i, block):
            inj1[g * 8 + i] = block.astype(BF16)

        inject(lambda j: blocks[j], 128, pts1, g * 8, 8, store)
        return carry

    lax.fori_loop(0, 4, inject_one, 0)
    load_t1.wait()

    def products(peer, half):
        def one(k, carry):
            w = t1[s_slot[peer, 0, k]]
            prod[peer * 32 + k] = lax.dot_general(got[peer, k], w, NT, preferred_element_type=F32)
            return carry

        lax.fori_loop(half * 16, half * 16 + 16, one, 0, unroll=8)

    for half in range(2):
        products(col, half)
        for dx, dy in ORDER:
            peer = at(4 - dx, 4 - dy)
            part = pl.ds(half * 16, 16)
            remote(
                snd.at[peer, part], got.at[peer, part], rep_s.at[peer, half], rep_r.at[peer, half], col=peer
            ).wait_recv()
            products(peer, half)

    zero = jnp.zeros((V, E), F32)
    run[0] = zero

    def add_one(s, total):
        total = total + prod[s_tgt[0, s]]
        run[s + 1] = total
        return total

    lax.fori_loop(0, t1.shape[0], add_one, zero, unroll=8)

    def sums(ptr, b):
        return run[ptr[b + 1]] - run[ptr[b]]

    for dz in (1, 3, 2, 0):
        zt = lax.rem(z + dz, 4)

        def give(i, carry, zt=zt):
            d_snd[zt, i] = sums(ptr1, zt * 64 + other * 32 + i).astype(BF16)
            return carry

        lax.fori_loop(0, 32, give, 0, unroll=8)
        remote(d_snd.at[zt], d_got.at[zt], d_s.at[zt], d_r.at[zt], row=z * 2 + other).start()
    for dz in (1, 3, 2, 0):
        zt = lax.rem(z + dz, 4)

        def keep(i, carry, zt=zt):
            own1[zt, i] = sums(ptr1, zt * 64 + core * 32 + i)
            return carry

        lax.fori_loop(0, 32, keep, 0, unroll=8)
    for dz in (1, 3, 2):
        zt = lax.rem(z + dz, 4)
        remote(d_snd.at[zt], d_got.at[zt], d_s.at[zt], d_r.at[zt], row=z * 2 + other).wait_recv()

        def join(i, carry, zt=zt):
            z_snd[zt, i] = (own1[zt, i] + d_got[zt, i].astype(F32)).astype(BF16)
            return carry

        lax.fori_loop(0, 32, join, 0, unroll=8)
        remote(z_snd.at[zt], z_got.at[z], z_s.at[zt], z_r.at[z], row=zt * 2 + core).start()
    remote(d_snd.at[z], d_got.at[z], d_s.at[z], d_r.at[z], row=z * 2 + other).wait_recv()

    def base(i, carry):
        own1[z, i] = own1[z, i] + d_got[z, i].astype(F32) + inj1[i].astype(F32)
        return carry

    lax.fori_loop(0, 32, base, 0, unroll=8)
    for dz in (1, 3, 2):
        zt = lax.rem(z + dz, 4)
        remote(z_snd.at[zt], z_got.at[zt], z_s.at[zt], z_r.at[zt], row=zt * 2 + core).wait_recv()
    za, zb, zc = lax.rem(z + 1, 4), lax.rem(z + 3, 4), lax.rem(z + 2, 4)

    def final_one(i, carry):
        total = own1[z, i] + (
            (z_got[za, i].astype(F32) + z_got[zb, i].astype(F32)) + z_got[zc, i].astype(F32)
        )
        block = total.astype(BF16)
        g1[row * 32 + i] = block
        out1[:, pl.ds(pl.multiple_of(i * E, E), E)] = block
        return carry

    lax.fori_loop(0, 32, final_one, 0, unroll=8)

    def piece(r):
        return g1.at[pl.ds(r * 32, 32)]

    for dz in (1, 3, 2):
        zt = lax.rem(z + dz, 4)
        remote(piece(row), piece(row), a_s.at[zt, 0], a_r.at[row], row=zt * 2 + core).start()
    remote(piece(row), piece(row), a_s.at[z, 1], a_r.at[row], row=z * 2 + other).start()
    write1 = pltpu.make_async_copy(out1, out1_hbm, o_sem.at[0])
    write1.start()

    def store2(i, block):
        inj2[i] = block

    inject(lambda j: g1[row * 32 + j], 32, pts2, 0, 8, store2)
    load_t2.wait()
    for dz in (1, 3, 2):
        zt = lax.rem(z + dz, 4)
        r = zt * 2 + core
        remote(piece(r), piece(r), a_s.at[zt, 0], a_r.at[r], row=r).wait_recv()
        remote(piece(r), piece(r), a_s.at[zt, 1], a_r.at[r], row=z * 2 + other).start()
    for dz in (0, 1, 3, 2):
        zt = lax.rem(z + dz, 4)
        r = zt * 2 + other
        remote(piece(r), piece(r), a_s.at[zt, 1], a_r.at[r], row=z * 2 + other).wait_recv()

    def slot_two(s, total):
        w = t2[s]
        total = total + lax.dot_general(g1[cols2[s]], w, NT, preferred_element_type=F32)
        run[s + 1] = total
        return total

    lax.fori_loop(0, t2.shape[0], slot_two, zero, unroll=8)
    for dx, dy in ORDER:
        peer = at(dx, dy)

        def give2(i, carry, peer=peer):
            c_snd[peer, i] = sums(ptr2, peer * 8 + i).astype(BF16)
            return carry

        lax.fori_loop(0, 8, give2, 0, unroll=8)
        remote(c_snd.at[peer], c_got.at[col], p_s.at[peer], p_r.at[col], col=peer).start()

    for i in range(8):
        own2[i] = sums(ptr2, col * 8 + i) + inj2[i]
    for dx, dy in ORDER:
        peer = at(4 - dx, 4 - dy)
        remote(c_snd.at[peer], c_got.at[peer], p_s.at[peer], p_r.at[peer], col=peer).wait_recv()

    def final_two(i, carry):
        total = own2[i]
        for dx, dy in ORDER:
            total = total + c_got[at(dx, dy), i].astype(F32)
        block = total.astype(BF16)
        g2[col * 8 + i] = block
        out2[:, pl.ds(pl.multiple_of(i * E, E), E)] = block
        return carry

    lax.fori_loop(0, 8, final_two, 0)

    def piece2(c):
        return g2.at[pl.ds(c * 8, 8)]

    for dx, dy in ORDER:
        peer = at(dx, dy)
        remote(piece2(col), piece2(col), q_s.at[peer], q_r.at[col], col=peer).start()
    write2 = pltpu.make_async_copy(out2, out2_hbm, o_sem.at[1])
    write2.start()

    held = []

    def store3(i, block):
        held.append(block)

    inject(lambda j: g2[col * 8 + j], 8, pts3, 0, 2, store3)
    load_t3.wait()
    for dx, dy in ORDER:
        peer = at(4 - dx, 4 - dy)
        remote(piece2(peer), piece2(peer), q_s.at[peer], q_r.at[peer], col=peer).wait_recv()

    def slot_three(s, total):
        w = t3[s]
        total = total + lax.dot_general(g2[cols3[s]], w, NT, preferred_element_type=F32)
        run[s + 1] = total
        return total

    lax.fori_loop(0, t3.shape[0], slot_three, zero, unroll=8)
    for d in range(1, 8):
        peer = lax.rem(row + d, 8)
        for i in range(2):
            r_snd[peer, i] = sums(ptr3, peer * 2 + i).astype(BF16)
        remote(r_snd.at[peer], r_got.at[row], m_s.at[peer], m_r.at[row], row=peer).start()
    held = [held[i] + sums(ptr3, row * 2 + i) for i in range(2)]
    for d in range(1, 8):
        peer = lax.rem(row + d, 8)
        remote(r_snd.at[peer], r_got.at[peer], m_s.at[peer], m_r.at[peer], row=peer).wait_recv()
        held = [held[i] + r_got[peer, i].astype(F32) for i in range(2)]
    for i in range(2):
        out3[:, i * E : (i + 1) * E] = held[i].astype(BF16)
    write3 = pltpu.make_async_copy(out3, out3_hbm, o_sem.at[2])
    write3.start()

    for copy in asks:
        copy.wait_send()
    for copy in replies:
        copy.wait_send()
    for zt in range(4):
        remote(d_snd.at[zt], d_got.at[zt], d_s.at[zt], d_r.at[zt], row=z * 2 + other).wait_send()
    for dz in (1, 2, 3):
        zt = lax.rem(z + dz, 4)
        r = zt * 2 + core
        remote(z_snd.at[zt], z_got.at[z], z_s.at[zt], z_r.at[z], row=r).wait_send()
        remote(piece(row), piece(row), a_s.at[zt, 0], a_r.at[row], row=r).wait_send()
    for zt in range(4):
        r = zt * 2 + core
        remote(piece(r), piece(r), a_s.at[zt, 1], a_r.at[r], row=z * 2 + other).wait_send()
    for dx, dy in ORDER:
        peer = at(dx, dy)
        remote(c_snd.at[peer], c_got.at[col], p_s.at[peer], p_r.at[col], col=peer).wait_send()
        remote(piece2(col), piece2(col), q_s.at[peer], q_r.at[col], col=peer).wait_send()
    for d in range(1, 8):
        peer = lax.rem(row + d, 8)
        remote(r_snd.at[peer], r_got.at[row], m_s.at[peer], m_r.at[row], row=peer).wait_send()
    write1.wait()
    write2.wait()
    write3.wait()


def on_device(
    fine, tiles1, ptr1, cols1, pts1, tiles2, ptr2, cols2, pts2, tiles3, ptr3, cols3, pts3
):
    n1, n2, n3 = tiles1.shape[0], tiles2.shape[0], tiles3.shape[0]
    hbm = pl.BlockSpec(memory_space=pl.ANY)
    vmem = pl.BlockSpec(memory_space=pltpu.VMEM)
    smem = pl.BlockSpec(memory_space=pltpu.SMEM)
    dma = pltpu.SemaphoreType.DMA
    outs = [
        jax.ShapeDtypeStruct((V, pts1.shape[0]), BF16),
        jax.ShapeDtypeStruct((V, pts2.shape[0]), BF16),
        jax.ShapeDtypeStruct((V, pts3.shape[0]), BF16),
    ]
    vm = pltpu.VMEM
    scratch = [
        vm(fine.shape, BF16), vm((128, V, E), BF16), vm(tiles1.shape, BF16), vm(tiles2.shape, BF16), vm(tiles3.shape, BF16),
        vm((16, 1, E), I32), pltpu.SMEM((16, 1, E), I32),
        vm((16, 32, V, E), BF16), vm((16, 32, V, E), BF16), vm((n1, V, E), F32), vm((n1 + 1, V, E), F32),
        vm((4, 32, V, E), BF16), vm((4, 32, V, E), BF16), vm((4, 32, V, E), F32),
        vm((4, 32, V, E), BF16), vm((4, 32, V, E), BF16), vm((32, V, E), BF16), vm((256, V, E), BF16),
        vm((16, 8, V, E), BF16), vm((16, 8, V, E), BF16), vm((8, V, E), F32), vm((8, V, E), F32), vm((128, V, E), BF16),
        vm((8, 2, V, E), BF16), vm((8, 2, V, E), BF16),
        vm(outs[0].shape, BF16), vm(outs[1].shape, BF16), vm(outs[2].shape, BF16),
        dma((1,)), dma((3,)), dma((1,)),
        dma((16,)), dma((16,)), dma((16, 2)), dma((16, 2)), dma((4,)), dma((4,)), dma((4,)), dma((4,)), dma((4, 2)), dma((8,)),
        dma((16,)), dma((16,)), dma((16,)), dma((16,)), dma((8,)), dma((8,)), dma((3,)),
    ]
    ask, slot, tgt = pl.pallas_call(
        plan,
        out_shape=[
            jax.ShapeDtypeStruct((16, 1, E), I32),
            jax.ShapeDtypeStruct((16, 1, E), I32),
            jax.ShapeDtypeStruct((1, n1), I32),
        ],
        in_specs=[smem, vmem],
        out_specs=[vmem] * 3,
        name="plan",
    )(ptr1, cols1.reshape(1, n1))
    return pl.pallas_call(
        kernel,
        out_shape=outs,
        in_specs=[vmem] * 4 + [smem] * 7 + [hbm] * 4,
        out_specs=[hbm] * 3,
        scratch_shapes=scratch,
        compiler_params=pltpu.CompilerParams(
            collective_id=0, has_side_effects=True, vmem_limit_bytes=58 << 20
        ),
        name="restrict",
    )(
        ask, pts1.reshape(-1, E), pts2.reshape(-1, E), pts3.reshape(-1, E),
        tgt, slot, ptr1, cols2, ptr2, cols3, ptr3, fine, tiles1, tiles2, tiles3,
    )


def solution(mesh):
    placed = (
        P(None, ("row", "col")),
        P(("row", "col"), None, None),
        P(("row", "col")),
        P(("row", "col")),
        P(("col", "row")),
        P(("row", "col"), None, None),
        P(("row", "col")),
        P(("row", "col")),
        P(("row", "col")),
        P(("row", "col"), None, None),
        P(("row", "col")),
        P(("row", "col")),
        P(("col", "row")),
    )
    return jax.shard_map(
        on_device,
        mesh=mesh,
        in_specs=placed,
        out_specs=(P(None, ("col", "row")), P(None, ("row", "col")), P(None, ("col", "row"))),
        check_vma=False,
    )
```

```python
import jax
import jax.numpy as jnp
from jax import lax
from jax.experimental import pallas as pl
from jax.experimental.pallas import tpu as pltpu
from jax.sharding import PartitionSpec as P

MESH = pl.DeviceIdType.MESH
F32 = jnp.float32
BF16 = jnp.bfloat16
I32 = jnp.int32
E = 128
V = 16
ORDER = (
    (1, 1), (3, 3), (0, 2), (1, 3), (3, 1), (2, 0), (1, 2), (3, 2),
    (2, 1), (2, 3), (0, 1), (0, 3), (1, 0), (3, 0), (2, 2),
)
H = 8
NEG = tuple(ORDER.index(((4 - dx) % 4, (4 - dy) % 4)) for dx, dy in ORDER)
NT = (((1,), (1,)), ((), ()))


def at(col, offset):
    return lax.rem(col // 4 + offset[1], 4) * 4 + lax.rem(lax.rem(col, 4) + offset[0], 4)


def inject(load, n_src, points, first, group, store):
    low, high = [], []
    rows = load(0).shape[0]
    for i in range(group):
        line = jnp.broadcast_to(points[pl.ds(first + i, 1), :], (rows, E))
        low.append(line & (E - 1))
        high.append(line >> 7)

    def source(j, held):
        block = load(j).astype(F32)
        return tuple(
            jnp.where(
                high[i] == j,
                jnp.take_along_axis(block, low[i], axis=1, mode="promise_in_bounds"),
                held[i],
            )
            for i in range(group)
        )

    zero = jnp.zeros((rows, E), F32)
    held = lax.fori_loop(0, n_src, source, (zero,) * group, unroll=8)
    for i in range(group):
        store(i, held[i])


def pair_products(x, other_x, w, other_w):
    none = jnp.zeros_like(x)
    lhs = jnp.concatenate(
        [jnp.concatenate([x, none], axis=1), jnp.concatenate([none, other_x], axis=1)], axis=0
    )
    both = lax.dot_general(
        lhs, jnp.concatenate([w, other_w], axis=1), NT, preferred_element_type=F32
    )
    return both[:H], both[H:]


def plan(ptr1, cols1, ask, slot, tgt):
    col = lax.axis_index("col")
    n1 = cols1.shape[1]
    live = ptr1[ptr1.shape[0] - 1]
    names = cols1[...]
    lanes = lax.broadcasted_iota(I32, (1, n1), 1)
    owner = names >> 7
    hit = jnp.where(
        (lax.broadcasted_iota(I32, (16, n1), 0) == owner) & (lanes < live), 1.0, 0.0
    ).astype(F32)
    before = jnp.where(
        lax.broadcasted_iota(I32, (n1, n1), 0) < lax.broadcasted_iota(I32, (n1, n1), 1), 1.0, 0.0
    ).astype(BF16)
    count = jnp.dot(hit.astype(BF16), before, preferred_element_type=F32)
    rank = jnp.sum(hit * count, axis=0, keepdims=True)
    line = jnp.full((1, n1), 15, I32)
    for i in range(15):
        line = jnp.where(owner == at(col, ORDER[NEG[i]]), i, line)
    tgt[...] = jnp.where(lanes < live, line * 32 + rank.astype(I32), 0)
    place = jnp.where(
        lax.broadcasted_iota(I32, (E, n1), 0).astype(F32) == rank, 1.0, 0.0
    ).astype(BF16)
    listed = jnp.concatenate(
        [
            hit * (names & (E - 1)).astype(F32),
            hit * (lanes >> 8).astype(F32),
            hit * (lanes & 255).astype(F32),
        ],
        axis=0,
    ).astype(BF16)
    table = lax.dot_general(listed, place, NT, preferred_element_type=F32).astype(I32)
    for p in range(16):
        ask[p] = table[p : p + 1]
        spot = jnp.int32(15)
        for i in range(15):
            spot = jnp.where(at(col, ORDER[NEG[i]]) == p, i, spot)
        slot[spot] = table[16 + p : 17 + p] * 256 + table[32 + p : 33 + p]


def emit(parts, out1, out2, out3):
    first = 0
    for out in (out1, out2, out3):
        for i in range(out.shape[1] // E):
            out[:, i * E : (i + 1) * E] = jnp.concatenate(
                [parts[0, first + i], parts[1, first + i]], axis=0
            )
        first += out.shape[1] // E


def kernel(
    ask, pts1, pts2, pts3, s_tgt, s_slot, ptr1, cols2, ptr2, cols3, ptr3,
    fine_hbm, t1_hbm, t2_hbm, t3_hbm,
    parts_hbm,
    fine, blocks, t1, t2, t3,
    asked, s_asked,
    snd, got, prod, run,
    d_snd, d_got, own1, z_snd, z_got, inj1, g1a, g1b,
    c_snd, c_got, own2, inj2, g2a, g2b,
    r_snd, r_got, own3, out3,
    ld_sem, t_sem, ix_sem,
    ask_s, ask_r, rep_s, rep_r, d_s, d_r, z_s, z_r, a_s, a_r,
    p_s, p_r, q_s, q_r, m_s, m_r, o_sem,
):
    row = lax.axis_index("row")
    col = lax.axis_index("col")
    z, core = row // 2, lax.rem(row, 2)
    other = 1 - core
    partner = z * 2 + other
    g1, g2 = (g1a, g1b), (g2a, g2b)
    zero = jnp.zeros((H, E), F32)
    zs = [lax.rem(z + dz, 4) for dz in (1, 3, 2)]
    to = [at(col, offset) for offset in ORDER]
    back = [at(col, ORDER[NEG[i]]) for i in range(15)]

    def remote(src, dst, send, recv, **device):
        return pltpu.make_async_remote_copy(
            src_ref=src, dst_ref=dst, send_sem=send, recv_sem=recv,
            device_id=device, device_id_type=MESH,
        )

    load_fine = pltpu.make_async_copy(fine_hbm, fine, ld_sem.at[0])
    load_fine.start()
    load_t1 = pltpu.make_async_copy(t1_hbm, t1, t_sem.at[0])
    load_t1.start()
    load_t2 = pltpu.make_async_copy(t2_hbm, t2, t_sem.at[1])
    load_t3 = pltpu.make_async_copy(t3_hbm, t3, t_sem.at[2])

    barrier = pltpu.get_barrier_semaphore()
    for d in range(1, 16):
        pl.semaphore_signal(barrier, inc=1, device_id={"col": lax.rem(col + d, 16)}, device_id_type=MESH)
    for d in range(1, 8):
        pl.semaphore_signal(barrier, inc=1, device_id={"row": lax.rem(row + d, 8)}, device_id_type=MESH)
    pl.semaphore_wait(barrier, 22)

    asks = [remote(ask.at[to[i]], asked.at[i], ask_s.at[i], ask_r.at[i], col=to[i]) for i in range(15)]
    for copy in asks:
        copy.start()
    asked[15] = ask[col]
    load_fine.wait()

    def cut(j, carry):
        block = fine[:, pl.ds(pl.multiple_of(j * E, E), E)].astype(F32)
        blocks[0, j] = block[:H].astype(BF16)
        blocks[1, j] = block[H:].astype(BF16)
        return carry

    lax.fori_loop(0, 128, cut, 0, unroll=8)
    for copy in asks:
        copy.wait_recv()
    copy_asked = pltpu.make_async_copy(asked, s_asked, ix_sem.at[0])
    copy_asked.start()
    copy_asked.wait()

    def fill(h, target, i):
        def one(k, carry):
            target[k] = blocks[h, s_asked[i, 0, k]]
            return carry

        lax.fori_loop(0, 32, one, 0, unroll=16)

    def reply(h, i):
        return remote(snd.at[h, i], got.at[h, i], rep_s.at[h, i], rep_r.at[h, i], col=to[i])

    for h in range(2):
        for i in range(15):
            fill(h, snd.at[h, i], NEG[i])
            reply(h, i).start()
    for h in range(2):
        fill(h, got.at[h, 15], 15)
    load_t2.start()
    load_t3.start()

    def inject_one(first, last):
        def some(g, carry):
            def store(i, block):
                inj1[0, g * 8 + i] = block[:H]
                inj1[1, g * 8 + i] = block[H:]

            inject(lambda j: fine[:, pl.ds(pl.multiple_of(j * E, E), E)], 128, pts1, g * 8, 8, store)
            return carry

        lax.fori_loop(first, last, some, 0)

    def products(h, first, last):
        for i in range(first, min(last, 15)):
            reply(h, i).wait_recv()

        def one(n, carry):
            i, k = n // 16, lax.rem(n, 16) * 2
            t = i * 32 + k
            prod[t], prod[t + 1] = pair_products(
                got[h, i, k], got[h, i, k + 1], t1[s_slot[i, 0, k]], t1[s_slot[i, 0, k + 1]]
            )
            return carry

        lax.fori_loop(first * 16, last * 16, one, 0, unroll=16)

    def sums(ptr, b):
        return run[ptr[b + 1]] - run[ptr[b]]

    def to_partner(h, zt):
        return remote(d_snd.at[h, zt], d_got.at[h, zt], d_s.at[h, zt], d_r.at[h, zt], row=partner)

    def along_z(h, i):
        j = (1, 0, 2)[i]
        return remote(z_snd.at[h, i], z_got.at[h, j], z_s.at[h, i], z_r.at[h, j], row=zs[i] * 2 + core)

    def sum_one(h):
        run[0] = zero

        def add(s, total):
            total = total + prod[s_tgt[0, s]]
            run[s + 1] = total
            return total

        lax.fori_loop(0, t1.shape[0], add, zero, unroll=16)
        for zt in zs + [z]:

            def give(i, carry, zt=zt):
                d_snd[h, zt, i] = sums(ptr1, zt * 64 + other * 32 + i).astype(BF16)
                return carry

            lax.fori_loop(0, 32, give, 0, unroll=16)
            to_partner(h, zt).start()
        for zt in zs + [z]:

            def keep(i, carry, zt=zt):
                own1[h, zt, i] = sums(ptr1, zt * 64 + core * 32 + i)
                return carry

            lax.fori_loop(0, 32, keep, 0, unroll=16)

    def join(h):
        for n, zt in enumerate(zs):
            to_partner(h, zt).wait_recv()

            def add(i, carry, zt=zt, n=n):
                z_snd[h, n, i] = (own1[h, zt, i] + d_got[h, zt, i].astype(F32)).astype(BF16)
                return carry

            lax.fori_loop(0, 32, add, 0, unroll=16)
            along_z(h, n).start()
        to_partner(h, z).wait_recv()

    def piece(h, r):
        return g1[h].at[pl.ds(r * 32, 32)]

    def spread_z(h, i):
        return remote(piece(h, row), piece(h, row), a_s.at[h, i], a_r.at[h, row], row=zs[i] * 2 + core)

    def spread_chip(h, zt, i):
        r = zt * 2 + core
        return remote(piece(h, r), piece(h, r), a_s.at[h, 3 + i], a_r.at[h, r], row=partner)

    def arrival(h, r):
        return remote(piece(h, r), piece(h, r), a_s.at[h, 0], a_r.at[h, r], row=partner)

    def final_one(h):
        for i in range(3):
            along_z(h, i).wait_recv()

        def add(i, carry):
            total = (own1[h, z, i] + d_got[h, z, i].astype(F32)) + inj1[h, i]
            for n in range(3):
                total = total + z_got[h, n, i].astype(F32)
            g1[h][row * 32 + i] = total.astype(BF16)
            return carry

        lax.fori_loop(0, 32, add, 0, unroll=16)
        for i in range(3):
            spread_z(h, i).start()
        spread_chip(h, z, 3).start()
        pltpu.make_async_copy(piece(h, row), parts_hbm.at[h, pl.ds(0, 32)], o_sem.at[h, 0]).start()

        def store(i, block):
            inj2[h, i] = block

        inject(lambda j: g1[h][row * 32 + j], 32, pts2, 0, 8, store)

    def pass_on(h):
        for i, zt in enumerate(zs):
            arrival(h, zt * 2 + core).wait_recv()
            spread_chip(h, zt, i).start()

    def arrived(h):
        for zt in [z] + zs:
            arrival(h, zt * 2 + other).wait_recv()

    def tile_sums(vectors, tiles, columns):
        run[0] = zero

        def two(n, total):
            s = n * 2
            a, b = pair_products(vectors[columns[s]], vectors[columns[s + 1]], tiles[s], tiles[s + 1])
            a = total + a
            run[s + 1] = a
            b = a + b
            run[s + 2] = b
            return b

        lax.fori_loop(0, tiles.shape[0] // 2, two, zero, unroll=16)

    def part_two(h, i):
        return remote(c_snd.at[h, i], c_got.at[h, i], p_s.at[h, i], p_r.at[h, i], col=to[i])

    def level_two(h):
        tile_sums(g1[h], t2, cols2)
        for n in range(15):

            def give(i, carry, n=n):
                c_snd[h, n, i] = sums(ptr2, to[n] * 8 + i).astype(BF16)
                return carry

            lax.fori_loop(0, 8, give, 0, unroll=8)
            part_two(h, n).start()

        def keep(i, carry):
            own2[h, i] = sums(ptr2, col * 8 + i) + inj2[h, i]
            return carry

        lax.fori_loop(0, 8, keep, 0, unroll=8)

    def spread_two(h, i):
        mine = g2[h].at[pl.ds(col * 8, 8)]
        return remote(mine, mine, q_s.at[h, i], q_r.at[h, i], col=to[i])

    def final_two(h):
        for i in range(15):
            part_two(h, i).wait_recv()

        def add(i, carry):
            total = own2[h, i]
            for n in range(15):
                total = total + c_got[h, n, i].astype(F32)
            g2[h][col * 8 + i] = total.astype(BF16)
            return carry

        lax.fori_loop(0, 8, add, 0, unroll=4)
        for i in range(15):
            spread_two(h, i).start()
        pltpu.make_async_copy(
            g2[h].at[pl.ds(col * 8, 8)], parts_hbm.at[h, pl.ds(32, 8)], o_sem.at[h, 1]
        ).start()

        def store(i, block):
            own3[h, i] = block

        inject(lambda j: g2[h][col * 8 + j], 8, pts3, 0, 2, store)

    def part_three(h, d):
        peer = lax.rem(row + d, 8)
        return remote(r_snd.at[h, d], r_got.at[h, d], m_s.at[h, d], m_r.at[h, d], row=peer)

    def level_three(h):
        for i in range(15):
            there = g2[h].at[pl.ds(back[i] * 8, 8)]
            remote(there, there, q_s.at[h, i], q_r.at[h, i], col=to[i]).wait_recv()
        tile_sums(g2[h], t3, cols3)
        for d in range(1, 8):
            peer = lax.rem(row + d, 8)
            for i in range(2):
                r_snd[h, d, i] = sums(ptr3, peer * 2 + i)
            part_three(h, d).start()
        for i in range(2):
            own3[h, i] = own3[h, i] + sums(ptr3, row * 2 + i)

    def final_three(h):
        for d in range(1, 8):
            part_three(h, d).wait_recv()
        for i in range(2):
            total = own3[h, i]
            for d in range(1, 8):
                total = total + r_got[h, d, i]
            out3[h, i] = total.astype(BF16)
        pltpu.make_async_copy(out3.at[h], parts_hbm.at[h, pl.ds(40, 2)], o_sem.at[h, 2]).start()

    A, B = 0, 1
    inject_one(0, 2)
    load_t1.wait()
    products(A, 0, 5)
    products(A, 5, 10)
    products(A, 10, 14)
    products(A, 14, 16)
    sum_one(A)
    products(B, 0, 3)
    join(A)
    inject_one(2, 4)
    final_one(A)
    products(B, 3, 9)
    products(B, 9, 14)
    pass_on(A)
    products(B, 14, 16)
    sum_one(B)
    join(B)
    load_t2.wait()
    arrived(A)
    level_two(A)
    final_one(B)
    final_two(A)
    pass_on(B)
    arrived(B)
    load_t3.wait()
    level_two(B)
    level_three(A)
    final_two(B)
    level_three(B)
    final_three(A)
    final_three(B)

    for copy in asks:
        copy.wait_send()
    for h in range(2):
        for i in range(15):
            reply(h, i).wait_send()
            part_two(h, i).wait_send()
            spread_two(h, i).wait_send()
        for zt in range(4):
            to_partner(h, zt).wait_send()
        for i, zt in enumerate(zs + [z]):
            spread_chip(h, zt, i).wait_send()
        for i in range(3):
            along_z(h, i).wait_send()
            spread_z(h, i).wait_send()
        for d in range(1, 8):
            part_three(h, d).wait_send()
        pltpu.make_async_copy(piece(h, row), parts_hbm.at[h, pl.ds(0, 32)], o_sem.at[h, 0]).wait()
        pltpu.make_async_copy(
            g2[h].at[pl.ds(col * 8, 8)], parts_hbm.at[h, pl.ds(32, 8)], o_sem.at[h, 1]
        ).wait()
        pltpu.make_async_copy(out3.at[h], parts_hbm.at[h, pl.ds(40, 2)], o_sem.at[h, 2]).wait()


def on_device(
    fine, tiles1, ptr1, cols1, pts1, tiles2, ptr2, cols2, pts2, tiles3, ptr3, cols3, pts3
):
    n1 = tiles1.shape[0]
    hbm = pl.BlockSpec(memory_space=pl.ANY)
    vmem = pl.BlockSpec(memory_space=pltpu.VMEM)
    smem = pl.BlockSpec(memory_space=pltpu.SMEM)
    dma = pltpu.SemaphoreType.DMA
    vm = pltpu.VMEM
    ask, slot, tgt = pl.pallas_call(
        plan,
        out_shape=[
            jax.ShapeDtypeStruct((16, 1, E), I32),
            jax.ShapeDtypeStruct((16, 1, E), I32),
            jax.ShapeDtypeStruct((1, n1), I32),
        ],
        in_specs=[smem, vmem],
        out_specs=[vmem] * 3,
        name="plan",
    )(ptr1, cols1.reshape(1, n1))
    scratch = [
        vm(fine.shape, BF16), vm((2, 128, H, E), BF16), vm(tiles1.shape, BF16), vm(tiles2.shape, BF16), vm(tiles3.shape, BF16),
        vm((16, 1, E), I32), pltpu.SMEM((16, 1, E), I32),
        vm((2, 15, 32, H, E), BF16), vm((2, 16, 32, H, E), BF16), vm((n1, H, E), F32), vm((n1 + 1, H, E), F32),
        vm((2, 4, 32, H, E), BF16), vm((2, 4, 32, H, E), BF16), vm((2, 4, 32, H, E), F32),
        vm((2, 3, 32, H, E), BF16), vm((2, 3, 32, H, E), BF16), vm((2, 32, H, E), F32), vm((256, H, E), BF16), vm((256, H, E), BF16),
        vm((2, 15, 8, H, E), BF16), vm((2, 15, 8, H, E), BF16), vm((2, 8, H, E), F32), vm((2, 8, H, E), F32), vm((128, H, E), BF16), vm((128, H, E), BF16),
        vm((2, 8, 2, H, E), F32), vm((2, 8, 2, H, E), F32), vm((2, 2, H, E), F32), vm((2, 2, H, E), BF16),
        dma((1,)), dma((3,)), dma((1,)),
        dma((15,)), dma((15,)), dma((2, 15)), dma((2, 15)), dma((2, 4)), dma((2, 4)), dma((2, 3)), dma((2, 3)), dma((2, 7)), dma((2, 8)),
        dma((2, 15)), dma((2, 15)), dma((2, 15)), dma((2, 15)), dma((2, 8)), dma((2, 8)), dma((2, 3)),
    ]
    parts = pl.pallas_call(
        kernel,
        out_shape=jax.ShapeDtypeStruct((2, 42, H, E), BF16),
        in_specs=[vmem] * 4 + [smem] * 7 + [hbm] * 4,
        out_specs=hbm,
        scratch_shapes=scratch,
        compiler_params=pltpu.CompilerParams(
            collective_id=0, has_side_effects=True, vmem_limit_bytes=58 << 20
        ),
        name="restrict",
    )(
        ask, pts1.reshape(-1, E), pts2.reshape(-1, E), pts3.reshape(-1, E),
        tgt, slot, ptr1, cols2, ptr2, cols3, ptr3, fine, tiles1, tiles2, tiles3,
    )
    return pl.pallas_call(
        emit,
        out_shape=tuple(
            jax.ShapeDtypeStruct((V, points.shape[0]), BF16) for points in (pts1, pts2, pts3)
        ),
        in_specs=[vmem],
        out_specs=(vmem,) * 3,
        name="emit",
    )(parts)


def solution(mesh):
    placed = (
        P(None, ("row", "col")),
        P(("row", "col"), None, None),
        P(("row", "col")),
        P(("row", "col")),
        P(("col", "row")),
        P(("row", "col"), None, None),
        P(("row", "col")),
        P(("row", "col")),
        P(("row", "col")),
        P(("row", "col"), None, None),
        P(("row", "col")),
        P(("row", "col")),
        P(("col", "row")),
    )
    return jax.shard_map(
        on_device,
        mesh=mesh,
        in_specs=placed,
        out_specs=(P(None, ("col", "row")), P(None, ("row", "col")), P(None, ("col", "row"))),
        check_vma=False,
    )
```

```python
import jax
import jax.numpy as jnp
from jax import lax
from jax.experimental import pallas as pl
from jax.experimental.pallas import tpu as pltpu
from jax.sharding import PartitionSpec as P

MESH = pl.DeviceIdType.MESH
F32 = jnp.float32
BF16 = jnp.bfloat16
I32 = jnp.int32
E = 128
V = 16
ORDER = (
    (1, 1), (3, 3), (0, 2), (1, 3), (3, 1), (2, 0), (1, 2), (3, 2),
    (2, 1), (2, 3), (0, 1), (0, 3), (1, 0), (3, 0), (2, 2),
)
H = 8
NEG = tuple(ORDER.index(((4 - dx) % 4, (4 - dy) % 4)) for dx, dy in ORDER)
NT = (((1,), (1,)), ((), ()))


def at(col, offset):
    return lax.rem(col // 4 + offset[1], 4) * 4 + lax.rem(lax.rem(col, 4) + offset[0], 4)


def inject(load, n_src, points, first, group, store):
    low, high = [], []
    rows = load(0).shape[0]
    for i in range(group):
        line = jnp.broadcast_to(points[pl.ds(first + i, 1), :], (rows, E))
        low.append(line & (E - 1))
        high.append(line >> 7)

    def source(j, held):
        block = load(j).astype(F32)
        return tuple(
            jnp.where(
                high[i] == j,
                jnp.take_along_axis(block, low[i], axis=1, mode="promise_in_bounds"),
                held[i],
            )
            for i in range(group)
        )

    zero = jnp.zeros((rows, E), F32)
    held = lax.fori_loop(0, n_src, source, (zero,) * group, unroll=8)
    for i in range(group):
        store(i, held[i])


def pair_products(x, other_x, w, other_w):
    none = jnp.zeros_like(x)
    lhs = jnp.concatenate(
        [jnp.concatenate([x, none], axis=1), jnp.concatenate([none, other_x], axis=1)], axis=0
    )
    both = lax.dot_general(
        lhs, jnp.concatenate([w, other_w], axis=1), NT, preferred_element_type=F32
    )
    return both[:H], both[H:]


def plan(ptr1, cols1, ask, slot, tgt):
    col = lax.axis_index("col")
    n1 = cols1.shape[1]
    live = ptr1[ptr1.shape[0] - 1]
    names = cols1[...]
    lanes = lax.broadcasted_iota(I32, (1, n1), 1)
    owner = names >> 7
    hit = jnp.where(
        (lax.broadcasted_iota(I32, (16, n1), 0) == owner) & (lanes < live), 1.0, 0.0
    ).astype(F32)
    before = jnp.where(
        lax.broadcasted_iota(I32, (n1, n1), 0) < lax.broadcasted_iota(I32, (n1, n1), 1), 1.0, 0.0
    ).astype(BF16)
    count = jnp.dot(hit.astype(BF16), before, preferred_element_type=F32)
    rank = jnp.sum(hit * count, axis=0, keepdims=True)
    line = jnp.full((1, n1), 15, I32)
    for i in range(15):
        line = jnp.where(owner == at(col, ORDER[NEG[i]]), i, line)
    tgt[...] = jnp.where(lanes < live, line * 32 + rank.astype(I32), 0)
    place = jnp.where(
        lax.broadcasted_iota(I32, (E, n1), 0).astype(F32) == rank, 1.0, 0.0
    ).astype(BF16)
    listed = jnp.concatenate(
        [
            hit * (names & (E - 1)).astype(F32),
            hit * (lanes >> 8).astype(F32),
            hit * (lanes & 255).astype(F32),
        ],
        axis=0,
    ).astype(BF16)
    table = lax.dot_general(listed, place, NT, preferred_element_type=F32).astype(I32)
    for p in range(16):
        ask[p] = table[p : p + 1]
        spot = jnp.int32(15)
        for i in range(15):
            spot = jnp.where(at(col, ORDER[NEG[i]]) == p, i, spot)
        slot[spot] = table[16 + p : 17 + p] * 256 + table[32 + p : 33 + p]


def emit(parts, out1, out2, out3):
    first = 0
    for out in (out1, out2, out3):
        for i in range(out.shape[1] // E):
            out[:, i * E : (i + 1) * E] = jnp.concatenate(
                [parts[0, first + i], parts[1, first + i]], axis=0
            )
        first += out.shape[1] // E


def kernel(
    ask, pts1, pts2, pts3, s_tgt, s_slot, ptr1, cols2, ptr2, cols3, ptr3,
    fine_hbm, t1_hbm, t2_hbm, t3_hbm,
    parts_hbm,
    fine, blocks, t1, t2, t3,
    s_asked,
    snd, got, prod, run,
    d_snd, d_got, own1, z_snd, z_got, inj1, g1a, g1b,
    c_snd, c_got, own2, inj2, g2a, g2b,
    r_snd, r_got, own3, out3,
    ld_sem, t_sem, ix_sem,
    ask_s, ask_r, rep_s, rep_r, d_s, d_r, z_s, z_r, a_s, a_r,
    p_s, p_r, q_s, q_r, m_s, m_r, o_sem,
):
    row = lax.axis_index("row")
    col = lax.axis_index("col")
    z, core = row // 2, lax.rem(row, 2)
    other = 1 - core
    partner = z * 2 + other
    g1, g2 = (g1a, g1b), (g2a, g2b)
    zero = jnp.zeros((H, E), F32)
    zs = [lax.rem(z + dz, 4) for dz in (1, 3, 2)]
    to = [at(col, offset) for offset in ORDER]
    back = [at(col, ORDER[NEG[i]]) for i in range(15)]

    def remote(src, dst, send, recv, **device):
        return pltpu.make_async_remote_copy(
            src_ref=src, dst_ref=dst, send_sem=send, recv_sem=recv,
            device_id=device, device_id_type=MESH,
        )

    load_fine = pltpu.make_async_copy(fine_hbm, fine, ld_sem.at[0])
    load_fine.start()
    load_t1 = pltpu.make_async_copy(t1_hbm, t1, t_sem.at[0])
    load_t1.start()
    load_t2 = pltpu.make_async_copy(t2_hbm, t2, t_sem.at[1])
    load_t3 = pltpu.make_async_copy(t3_hbm, t3, t_sem.at[2])

    barrier = pltpu.get_barrier_semaphore()
    for d in range(1, 16):
        pl.semaphore_signal(barrier, inc=1, device_id={"col": lax.rem(col + d, 16)}, device_id_type=MESH)
    for d in range(1, 8):
        pl.semaphore_signal(barrier, inc=1, device_id={"row": lax.rem(row + d, 8)}, device_id_type=MESH)
    pl.semaphore_wait(barrier, 22)

    asks = [remote(ask.at[to[i]], s_asked.at[i], ask_s.at[i], ask_r.at[i], col=to[i]) for i in range(15)]
    for copy in asks:
        copy.start()
    own_ask = pltpu.make_async_copy(ask.at[col], s_asked.at[15], ix_sem.at[0])
    own_ask.start()
    load_fine.wait()

    def cut(j, carry):
        block = fine[:, pl.ds(pl.multiple_of(j * E, E), E)].astype(F32)
        blocks[0, j] = block[:H].astype(BF16)
        blocks[1, j] = block[H:].astype(BF16)
        return carry

    lax.fori_loop(0, 128, cut, 0, unroll=8)
    for copy in asks:
        copy.wait_recv()
    own_ask.wait()

    def fill(h, target, i):
        def one(k, carry):
            target[k] = blocks[h, s_asked[i, 0, k]]
            return carry

        lax.fori_loop(0, 32, one, 0, unroll=16)

    def reply(h, i):
        return remote(snd.at[h, i], got.at[h, i], rep_s.at[h, i], rep_r.at[h, i], col=to[i])

    for h in range(2):
        for i in range(15):
            fill(h, snd.at[h, i], NEG[i])
            reply(h, i).start()
    for h in range(2):
        fill(h, got.at[h, 15], 15)
    load_t2.start()
    load_t3.start()

    def inject_one(first, last):
        def some(g, carry):
            def store(i, block):
                inj1[0, g * 8 + i] = block[:H]
                inj1[1, g * 8 + i] = block[H:]

            inject(lambda j: fine[:, pl.ds(pl.multiple_of(j * E, E), E)], 128, pts1, g * 8, 8, store)
            return carry

        lax.fori_loop(first, last, some, 0)

    def products(h, first, last):
        for i in range(first, min(last, 15)):
            reply(h, i).wait_recv()

        def one(n, carry):
            i, k = n // 16, lax.rem(n, 16) * 2
            t = i * 32 + k
            prod[t], prod[t + 1] = pair_products(
                got[h, i, k], got[h, i, k + 1], t1[s_slot[i, 0, k]], t1[s_slot[i, 0, k + 1]]
            )
            return carry

        lax.fori_loop(first * 16, last * 16, one, 0, unroll=16)

    def sums(ptr, b):
        return run[ptr[b + 1]] - run[ptr[b]]

    def to_partner(h, zt):
        return remote(d_snd.at[h, zt], d_got.at[h, zt], d_s.at[h, zt], d_r.at[h, zt], row=partner)

    def along_z(h, i):
        j = (1, 0, 2)[i]
        return remote(z_snd.at[h, i], z_got.at[h, j], z_s.at[h, i], z_r.at[h, j], row=zs[i] * 2 + core)

    def sum_one(h):
        run[0] = zero

        def add(s, total):
            total = total + prod[s_tgt[0, s]]
            run[s + 1] = total
            return total

        lax.fori_loop(0, t1.shape[0], add, zero, unroll=16)
        for zt in zs + [z]:

            def give(i, carry, zt=zt):
                d_snd[h, zt, i] = sums(ptr1, zt * 64 + other * 32 + i).astype(BF16)
                return carry

            lax.fori_loop(0, 32, give, 0, unroll=16)
            to_partner(h, zt).start()
        for zt in zs + [z]:

            def keep(i, carry, zt=zt):
                own1[h, zt, i] = sums(ptr1, zt * 64 + core * 32 + i)
                return carry

            lax.fori_loop(0, 32, keep, 0, unroll=16)

    def join(h):
        for n, zt in enumerate(zs):
            to_partner(h, zt).wait_recv()

            def add(i, carry, zt=zt, n=n):
                z_snd[h, n, i] = (own1[h, zt, i] + d_got[h, zt, i].astype(F32)).astype(BF16)
                return carry

            lax.fori_loop(0, 32, add, 0, unroll=16)
            along_z(h, n).start()
        to_partner(h, z).wait_recv()

    def piece(h, r):
        return g1[h].at[pl.ds(r * 32, 32)]

    def spread_z(h, i):
        return remote(piece(h, row), piece(h, row), a_s.at[h, i], a_r.at[h, row], row=zs[i] * 2 + core)

    def spread_chip(h, zt, i):
        r = zt * 2 + core
        return remote(piece(h, r), piece(h, r), a_s.at[h, 3 + i], a_r.at[h, r], row=partner)

    def arrival(h, r):
        return remote(piece(h, r), piece(h, r), a_s.at[h, 0], a_r.at[h, r], row=partner)

    def final_one(h):
        for i in range(3):
            along_z(h, i).wait_recv()

        def add(i, carry):
            total = (own1[h, z, i] + d_got[h, z, i].astype(F32)) + inj1[h, i]
            for n in range(3):
                total = total + z_got[h, n, i].astype(F32)
            g1[h][row * 32 + i] = total.astype(BF16)
            return carry

        lax.fori_loop(0, 32, add, 0, unroll=16)
        for i in range(3):
            spread_z(h, i).start()
        spread_chip(h, z, 3).start()
        pltpu.make_async_copy(piece(h, row), parts_hbm.at[h, pl.ds(0, 32)], o_sem.at[h, 0]).start()

        def store(i, block):
            inj2[h, i] = block

        inject(lambda j: g1[h][row * 32 + j], 32, pts2, 0, 8, store)

    def pass_on(h):
        for i, zt in enumerate(zs):
            arrival(h, zt * 2 + core).wait_recv()
            spread_chip(h, zt, i).start()

    def arrived(h):
        for zt in [z] + zs:
            arrival(h, zt * 2 + other).wait_recv()

    def tile_sums(vectors, tiles, columns):
        run[0] = zero

        def two(n, total):
            s = n * 2
            a, b = pair_products(vectors[columns[s]], vectors[columns[s + 1]], tiles[s], tiles[s + 1])
            a = total + a
            run[s + 1] = a
            b = a + b
            run[s + 2] = b
            return b

        lax.fori_loop(0, tiles.shape[0] // 2, two, zero, unroll=16)

    def part_two(h, i):
        return remote(c_snd.at[h, i], c_got.at[h, i], p_s.at[h, i], p_r.at[h, i], col=to[i])

    def level_two(h):
        tile_sums(g1[h], t2, cols2)
        for n in range(15):

            def give(i, carry, n=n):
                c_snd[h, n, i] = sums(ptr2, to[n] * 8 + i).astype(BF16)
                return carry

            lax.fori_loop(0, 8, give, 0, unroll=8)
            part_two(h, n).start()

        def keep(i, carry):
            own2[h, i] = sums(ptr2, col * 8 + i) + inj2[h, i]
            return carry

        lax.fori_loop(0, 8, keep, 0, unroll=8)

    def spread_two(h, i):
        mine = g2[h].at[pl.ds(col * 8, 8)]
        return remote(mine, mine, q_s.at[h, i], q_r.at[h, i], col=to[i])

    def final_two(h):
        for i in range(15):
            part_two(h, i).wait_recv()

        def add(i, carry):
            total = own2[h, i]
            for n in range(15):
                total = total + c_got[h, n, i].astype(F32)
            g2[h][col * 8 + i] = total.astype(BF16)
            return carry

        lax.fori_loop(0, 8, add, 0, unroll=4)
        for i in range(15):
            spread_two(h, i).start()
        pltpu.make_async_copy(
            g2[h].at[pl.ds(col * 8, 8)], parts_hbm.at[h, pl.ds(32, 8)], o_sem.at[h, 1]
        ).start()

        def store(i, block):
            own3[h, i] = block

        inject(lambda j: g2[h][col * 8 + j], 8, pts3, 0, 2, store)

    def part_three(h, d):
        peer = lax.rem(row + d, 8)
        return remote(r_snd.at[h, d], r_got.at[h, d], m_s.at[h, d], m_r.at[h, d], row=peer)

    def level_three(h):
        for i in range(15):
            there = g2[h].at[pl.ds(back[i] * 8, 8)]
            remote(there, there, q_s.at[h, i], q_r.at[h, i], col=to[i]).wait_recv()
        tile_sums(g2[h], t3, cols3)
        for d in range(1, 8):
            peer = lax.rem(row + d, 8)
            for i in range(2):
                r_snd[h, d, i] = sums(ptr3, peer * 2 + i)
            part_three(h, d).start()
        for i in range(2):
            own3[h, i] = own3[h, i] + sums(ptr3, row * 2 + i)

    def final_three(h):
        for d in range(1, 8):
            part_three(h, d).wait_recv()
        for i in range(2):
            total = own3[h, i]
            for d in range(1, 8):
                total = total + r_got[h, d, i]
            out3[h, i] = total.astype(BF16)
        pltpu.make_async_copy(out3.at[h], parts_hbm.at[h, pl.ds(40, 2)], o_sem.at[h, 2]).start()

    A, B = 0, 1
    inject_one(0, 3)
    load_t1.wait()
    products(A, 0, 5)
    products(A, 5, 10)
    products(A, 10, 14)
    products(A, 14, 16)
    sum_one(A)
    products(B, 0, 3)
    join(A)
    inject_one(3, 4)
    final_one(A)
    products(B, 3, 9)
    products(B, 9, 14)
    products(B, 14, 16)
    sum_one(B)
    pass_on(A)
    join(B)
    load_t2.wait()
    arrived(A)
    level_two(A)
    final_one(B)
    pass_on(B)
    final_two(A)
    arrived(B)
    load_t3.wait()
    level_two(B)
    level_three(A)
    final_two(B)
    level_three(B)
    final_three(A)
    final_three(B)

    for copy in asks:
        copy.wait_send()
    for h in range(2):
        for i in range(15):
            reply(h, i).wait_send()
            part_two(h, i).wait_send()
            spread_two(h, i).wait_send()
        for zt in range(4):
            to_partner(h, zt).wait_send()
        for i, zt in enumerate(zs + [z]):
            spread_chip(h, zt, i).wait_send()
        for i in range(3):
            along_z(h, i).wait_send()
            spread_z(h, i).wait_send()
        for d in range(1, 8):
            part_three(h, d).wait_send()
        pltpu.make_async_copy(piece(h, row), parts_hbm.at[h, pl.ds(0, 32)], o_sem.at[h, 0]).wait()
        pltpu.make_async_copy(
            g2[h].at[pl.ds(col * 8, 8)], parts_hbm.at[h, pl.ds(32, 8)], o_sem.at[h, 1]
        ).wait()
        pltpu.make_async_copy(out3.at[h], parts_hbm.at[h, pl.ds(40, 2)], o_sem.at[h, 2]).wait()


def on_device(
    fine, tiles1, ptr1, cols1, pts1, tiles2, ptr2, cols2, pts2, tiles3, ptr3, cols3, pts3
):
    n1 = tiles1.shape[0]
    hbm = pl.BlockSpec(memory_space=pl.ANY)
    vmem = pl.BlockSpec(memory_space=pltpu.VMEM)
    smem = pl.BlockSpec(memory_space=pltpu.SMEM)
    dma = pltpu.SemaphoreType.DMA
    vm = pltpu.VMEM
    ask, slot, tgt = pl.pallas_call(
        plan,
        out_shape=[
            jax.ShapeDtypeStruct((16, 1, E), I32),
            jax.ShapeDtypeStruct((16, 1, E), I32),
            jax.ShapeDtypeStruct((1, n1), I32),
        ],
        in_specs=[smem, vmem],
        out_specs=[vmem] * 3,
        name="plan",
    )(ptr1, cols1.reshape(1, n1))
    scratch = [
        vm(fine.shape, BF16), vm((2, 128, H, E), BF16), vm(tiles1.shape, BF16), vm(tiles2.shape, BF16), vm(tiles3.shape, BF16),
        pltpu.SMEM((16, 1, E), I32),
        vm((2, 15, 32, H, E), BF16), vm((2, 16, 32, H, E), BF16), vm((n1, H, E), F32), vm((n1 + 1, H, E), F32),
        vm((2, 4, 32, H, E), BF16), vm((2, 4, 32, H, E), BF16), vm((2, 4, 32, H, E), F32),
        vm((2, 3, 32, H, E), BF16), vm((2, 3, 32, H, E), BF16), vm((2, 32, H, E), F32), vm((256, H, E), BF16), vm((256, H, E), BF16),
        vm((2, 15, 8, H, E), BF16), vm((2, 15, 8, H, E), BF16), vm((2, 8, H, E), F32), vm((2, 8, H, E), F32), vm((128, H, E), BF16), vm((128, H, E), BF16),
        vm((2, 8, 2, H, E), F32), vm((2, 8, 2, H, E), F32), vm((2, 2, H, E), F32), vm((2, 2, H, E), BF16),
        dma((1,)), dma((3,)), dma((1,)),
        dma((15,)), dma((15,)), dma((2, 15)), dma((2, 15)), dma((2, 4)), dma((2, 4)), dma((2, 3)), dma((2, 3)), dma((2, 7)), dma((2, 8)),
        dma((2, 15)), dma((2, 15)), dma((2, 15)), dma((2, 15)), dma((2, 8)), dma((2, 8)), dma((2, 3)),
    ]
    parts = pl.pallas_call(
        kernel,
        out_shape=jax.ShapeDtypeStruct((2, 42, H, E), BF16),
        in_specs=[vmem] * 4 + [smem] * 7 + [hbm] * 4,
        out_specs=hbm,
        scratch_shapes=scratch,
        compiler_params=pltpu.CompilerParams(
            collective_id=0, has_side_effects=True, vmem_limit_bytes=58 << 20
        ),
        name="restrict",
    )(
        ask, pts1.reshape(-1, E), pts2.reshape(-1, E), pts3.reshape(-1, E),
        tgt, slot, ptr1, cols2, ptr2, cols3, ptr3, fine, tiles1, tiles2, tiles3,
    )
    return pl.pallas_call(
        emit,
        out_shape=tuple(
            jax.ShapeDtypeStruct((V, points.shape[0]), BF16) for points in (pts1, pts2, pts3)
        ),
        in_specs=[vmem],
        out_specs=(vmem,) * 3,
        name="emit",
    )(parts)


def solution(mesh):
    placed = (
        P(None, ("row", "col")),
        P(("row", "col"), None, None),
        P(("row", "col")),
        P(("row", "col")),
        P(("col", "row")),
        P(("row", "col"), None, None),
        P(("row", "col")),
        P(("row", "col")),
        P(("row", "col")),
        P(("row", "col"), None, None),
        P(("row", "col")),
        P(("row", "col")),
        P(("col", "row")),
    )
    return jax.shard_map(
        on_device,
        mesh=mesh,
        in_specs=placed,
        out_specs=(P(None, ("col", "row")), P(None, ("row", "col")), P(None, ("col", "row"))),
        check_vma=False,
    )
```

```python
import jax
import jax.numpy as jnp
from jax import lax
from jax.experimental import pallas as pl
from jax.experimental.pallas import tpu as pltpu
from jax.sharding import PartitionSpec as P

MESH = pl.DeviceIdType.MESH
F32 = jnp.float32
BF16 = jnp.bfloat16
I32 = jnp.int32
E = 128
V = 16
ORDER = (
    (1, 1), (3, 3), (0, 2), (1, 3), (3, 1), (2, 0), (1, 2), (3, 2),
    (2, 1), (2, 3), (0, 1), (0, 3), (1, 0), (3, 0), (2, 2),
)
H = 8
NEG = tuple(ORDER.index(((4 - dx) % 4, (4 - dy) % 4)) for dx, dy in ORDER)
NT = (((1,), (1,)), ((), ()))


def at(col, offset):
    return lax.rem(col // 4 + offset[1], 4) * 4 + lax.rem(lax.rem(col, 4) + offset[0], 4)


def inject(load, n_src, points, first, group, store):
    low, high = [], []
    rows = load(0).shape[0]
    for i in range(group):
        line = jnp.broadcast_to(points[pl.ds(first + i, 1), :], (rows, E))
        low.append(line & (E - 1))
        high.append(line >> 7)

    def source(j, held):
        block = load(j).astype(F32)
        return tuple(
            jnp.where(
                high[i] == j,
                jnp.take_along_axis(block, low[i], axis=1, mode="promise_in_bounds"),
                held[i],
            )
            for i in range(group)
        )

    zero = jnp.zeros((rows, E), F32)
    held = lax.fori_loop(0, n_src, source, (zero,) * group, unroll=8)
    for i in range(group):
        store(i, held[i])


def pair_products(x, other_x, w, other_w):
    none = jnp.zeros_like(x)
    lhs = jnp.concatenate(
        [jnp.concatenate([x, none], axis=1), jnp.concatenate([none, other_x], axis=1)], axis=0
    )
    both = lax.dot_general(
        lhs, jnp.concatenate([w, other_w], axis=1), NT, preferred_element_type=F32
    )
    return both[:H], both[H:]


def plan(ptr1, cols1, ask, slot, tgt):
    col = lax.axis_index("col")
    n1 = cols1.shape[1]
    live = ptr1[ptr1.shape[0] - 1]
    names = cols1[...]
    lanes = lax.broadcasted_iota(I32, (1, n1), 1)
    owner = names >> 7
    hit = jnp.where(
        (lax.broadcasted_iota(I32, (16, n1), 0) == owner) & (lanes < live), 1.0, 0.0
    ).astype(F32)
    before = jnp.where(
        lax.broadcasted_iota(I32, (n1, n1), 0) < lax.broadcasted_iota(I32, (n1, n1), 1), 1.0, 0.0
    ).astype(BF16)
    count = jnp.dot(hit.astype(BF16), before, preferred_element_type=F32)
    rank = jnp.sum(hit * count, axis=0, keepdims=True)
    line = jnp.full((1, n1), 15, I32)
    for i in range(15):
        line = jnp.where(owner == at(col, ORDER[NEG[i]]), i, line)
    tgt[...] = jnp.where(lanes < live, line * 32 + rank.astype(I32), 0)
    place = jnp.where(
        lax.broadcasted_iota(I32, (E, n1), 0).astype(F32) == rank, 1.0, 0.0
    ).astype(BF16)
    listed = jnp.concatenate(
        [
            hit * (names & (E - 1)).astype(F32),
            hit * (lanes >> 8).astype(F32),
            hit * (lanes & 255).astype(F32),
        ],
        axis=0,
    ).astype(BF16)
    table = lax.dot_general(listed, place, NT, preferred_element_type=F32).astype(I32)
    for p in range(16):
        ask[p] = table[p : p + 1]
        spot = jnp.int32(15)
        for i in range(15):
            spot = jnp.where(at(col, ORDER[NEG[i]]) == p, i, spot)
        slot[spot] = table[16 + p : 17 + p] * 256 + table[32 + p : 33 + p]


def emit(parts, out1, out2, out3):
    first = 0
    for out in (out1, out2, out3):
        for i in range(out.shape[1] // E):
            out[:, i * E : (i + 1) * E] = jnp.concatenate(
                [parts[0, first + i], parts[1, first + i]], axis=0
            )
        first += out.shape[1] // E


def kernel(
    ask, pts1, pts2, pts3, s_tgt, s_slot, ptr1, cols2, ptr2, cols3, ptr3,
    fine_hbm, t1_hbm, t2_hbm, t3_hbm,
    parts_hbm,
    fine, blocks, t1, t2, t3,
    s_asked,
    snd, got, prod, run,
    d_snd, d_got, own1, z_snd, z_got, inj1, g1a, g1b,
    c_snd, c_got, own2, inj2, g2a, g2b,
    r_snd, r_got, own3, out3,
    ld_sem, t_sem, ix_sem,
    ask_s, ask_r, rep_s, rep_r, d_s, d_r, z_s, z_r, a_s, a_r,
    p_s, p_r, q_s, q_r, m_s, m_r, o_sem,
):
    row = lax.axis_index("row")
    col = lax.axis_index("col")
    z, core = row // 2, lax.rem(row, 2)
    other = 1 - core
    partner = z * 2 + other
    g1, g2 = (g1a, g1b), (g2a, g2b)
    zero = jnp.zeros((H, E), F32)
    zs = [lax.rem(z + dz, 4) for dz in (1, 3, 2)]
    to = [at(col, offset) for offset in ORDER]
    back = [at(col, ORDER[NEG[i]]) for i in range(15)]

    def remote(src, dst, send, recv, **device):
        return pltpu.make_async_remote_copy(
            src_ref=src, dst_ref=dst, send_sem=send, recv_sem=recv,
            device_id=device, device_id_type=MESH,
        )

    load_fine = pltpu.make_async_copy(fine_hbm, fine, ld_sem.at[0])
    load_fine.start()
    load_t1 = pltpu.make_async_copy(t1_hbm, t1, t_sem.at[0])
    load_t1.start()
    load_t2 = pltpu.make_async_copy(t2_hbm, t2, t_sem.at[1])
    load_t3 = pltpu.make_async_copy(t3_hbm, t3, t_sem.at[2])

    barrier = pltpu.get_barrier_semaphore()
    for d in range(1, 16):
        pl.semaphore_signal(barrier, inc=1, device_id={"col": lax.rem(col + d, 16)}, device_id_type=MESH)
    for d in range(1, 8):
        pl.semaphore_signal(barrier, inc=1, device_id={"row": lax.rem(row + d, 8)}, device_id_type=MESH)
    pl.semaphore_wait(barrier, 22)

    asks = [remote(ask.at[to[i]], s_asked.at[i], ask_s.at[i], ask_r.at[i], col=to[i]) for i in range(15)]
    for copy in asks:
        copy.start()
    own_ask = pltpu.make_async_copy(ask.at[col], s_asked.at[15], ix_sem.at[0])
    own_ask.start()
    load_fine.wait()

    def cut(j, carry):
        block = fine[:, pl.ds(pl.multiple_of(j * E, E), E)].astype(F32)
        blocks[0, j] = block[:H].astype(BF16)
        blocks[1, j] = block[H:].astype(BF16)
        return carry

    lax.fori_loop(0, 128, cut, 0, unroll=8)
    for copy in asks:
        copy.wait_recv()
    own_ask.wait()

    def fill(h, target, i):
        def one(k, carry):
            target[k] = blocks[h, s_asked[i, 0, k]]
            return carry

        lax.fori_loop(0, 32, one, 0, unroll=16)

    def reply(h, i):
        return remote(snd.at[h, i], got.at[h, i], rep_s.at[h, i], rep_r.at[h, i], col=to[i])

    for h in range(2):
        for i in range(15):
            fill(h, snd.at[h, i], NEG[i])
            reply(h, i).start()
    for h in range(2):
        fill(h, got.at[h, 15], 15)
    load_t2.start()
    load_t3.start()

    def inject_one(first, last):
        def some(g, carry):
            def store(i, block):
                inj1[0, g * 8 + i] = block[:H]
                inj1[1, g * 8 + i] = block[H:]

            inject(lambda j: fine[:, pl.ds(pl.multiple_of(j * E, E), E)], 128, pts1, g * 8, 8, store)
            return carry

        lax.fori_loop(first, last, some, 0)

    def products(h, first, last):
        for i in range(first, min(last, 15)):
            reply(h, i).wait_recv()

        def one(n, carry):
            i, k = n // 16, lax.rem(n, 16) * 2
            t = i * 32 + k
            prod[t], prod[t + 1] = pair_products(
                got[h, i, k], got[h, i, k + 1], t1[s_slot[i, 0, k]], t1[s_slot[i, 0, k + 1]]
            )
            return carry

        lax.fori_loop(first * 16, last * 16, one, 0, unroll=16)

    def sums(ptr, b):
        return run[ptr[b + 1]] - run[ptr[b]]

    def to_partner(h, zt):
        return remote(d_snd.at[h, zt], d_got.at[h, zt], d_s.at[h, zt], d_r.at[h, zt], row=partner)

    def along_z(h, i):
        j = (1, 0, 2)[i]
        return remote(z_snd.at[h, i], z_got.at[h, j], z_s.at[h, i], z_r.at[h, j], row=zs[i] * 2 + core)

    def sum_one(h):
        run[0] = zero

        def add(s, total):
            total = total + prod[s_tgt[0, s]]
            run[s + 1] = total
            return total

        lax.fori_loop(0, t1.shape[0], add, zero, unroll=16)
        for zt in zs + [z]:

            def give(i, carry, zt=zt):
                d_snd[h, zt, i] = sums(ptr1, zt * 64 + other * 32 + i).astype(BF16)
                return carry

            lax.fori_loop(0, 32, give, 0, unroll=16)
            to_partner(h, zt).start()
        for zt in zs + [z]:

            def keep(i, carry, zt=zt):
                own1[h, zt, i] = sums(ptr1, zt * 64 + core * 32 + i)
                return carry

            lax.fori_loop(0, 32, keep, 0, unroll=16)

    def join(h):
        for n, zt in enumerate(zs):
            to_partner(h, zt).wait_recv()

            def add(i, carry, zt=zt, n=n):
                z_snd[h, n, i] = (own1[h, zt, i] + d_got[h, zt, i].astype(F32)).astype(BF16)
                return carry

            lax.fori_loop(0, 32, add, 0, unroll=16)
            along_z(h, n).start()
        to_partner(h, z).wait_recv()

    def piece(h, r):
        return g1[h].at[pl.ds(r * 32, 32)]

    def spread_z(h, i):
        return remote(piece(h, row), piece(h, row), a_s.at[h, i], a_r.at[h, row], row=zs[i] * 2 + core)

    def spread_chip(h, zt, i):
        r = zt * 2 + core
        return remote(piece(h, r), piece(h, r), a_s.at[h, 3 + i], a_r.at[h, r], row=partner)

    def arrival(h, r):
        return remote(piece(h, r), piece(h, r), a_s.at[h, 0], a_r.at[h, r], row=partner)

    def final_one(h):
        for i in range(3):
            along_z(h, i).wait_recv()

        def add(i, carry):
            total = (own1[h, z, i] + d_got[h, z, i].astype(F32)) + inj1[h, i]
            for n in range(3):
                total = total + z_got[h, n, i].astype(F32)
            g1[h][row * 32 + i] = total.astype(BF16)
            return carry

        lax.fori_loop(0, 32, add, 0, unroll=16)
        for i in range(3):
            spread_z(h, i).start()
        spread_chip(h, z, 3).start()
        pltpu.make_async_copy(piece(h, row), parts_hbm.at[h, pl.ds(0, 32)], o_sem.at[h, 0]).start()

        def store(i, block):
            inj2[h, i] = block

        inject(lambda j: g1[h][row * 32 + j], 32, pts2, 0, 8, store)

    def pass_on(h):
        for i, zt in enumerate(zs):
            arrival(h, zt * 2 + core).wait_recv()
            spread_chip(h, zt, i).start()

    def arrived(h):
        for zt in [z] + zs:
            arrival(h, zt * 2 + other).wait_recv()

    def tile_sums(vectors, tiles, columns):
        run[0] = zero

        def two(n, total):
            s = n * 2
            a, b = pair_products(vectors[columns[s]], vectors[columns[s + 1]], tiles[s], tiles[s + 1])
            a = total + a
            run[s + 1] = a
            b = a + b
            run[s + 2] = b
            return b

        lax.fori_loop(0, tiles.shape[0] // 2, two, zero, unroll=16)

    def part_two(h, i):
        return remote(c_snd.at[h, i], c_got.at[h, i], p_s.at[h, i], p_r.at[h, i], col=to[i])

    def level_two(h):
        tile_sums(g1[h], t2, cols2)
        for n in range(15):

            def give(i, carry, n=n):
                c_snd[h, n, i] = sums(ptr2, to[n] * 8 + i).astype(BF16)
                return carry

            lax.fori_loop(0, 8, give, 0, unroll=8)
            part_two(h, n).start()

        def keep(i, carry):
            own2[h, i] = sums(ptr2, col * 8 + i) + inj2[h, i]
            return carry

        lax.fori_loop(0, 8, keep, 0, unroll=8)

    def spread_two(h, i):
        mine = g2[h].at[pl.ds(col * 8, 8)]
        return remote(mine, mine, q_s.at[h, i], q_r.at[h, i], col=to[i])

    def final_two(h):
        for i in range(15):
            part_two(h, i).wait_recv()

        def add(i, carry):
            total = own2[h, i]
            for n in range(15):
                total = total + c_got[h, n, i].astype(F32)
            g2[h][col * 8 + i] = total.astype(BF16)
            return carry

        lax.fori_loop(0, 8, add, 0, unroll=4)
        for i in range(15):
            spread_two(h, i).start()
        pltpu.make_async_copy(
            g2[h].at[pl.ds(col * 8, 8)], parts_hbm.at[h, pl.ds(32, 8)], o_sem.at[h, 1]
        ).start()

        def store(i, block):
            own3[h, i] = block

        inject(lambda j: g2[h][col * 8 + j], 8, pts3, 0, 2, store)

    def part_three(h, d):
        peer = lax.rem(row + d, 8)
        return remote(r_snd.at[h, d], r_got.at[h, d], m_s.at[h, d], m_r.at[h, d], row=peer)

    def level_three(h):
        for i in range(15):
            there = g2[h].at[pl.ds(back[i] * 8, 8)]
            remote(there, there, q_s.at[h, i], q_r.at[h, i], col=to[i]).wait_recv()
        tile_sums(g2[h], t3, cols3)
        for d in range(1, 8):
            peer = lax.rem(row + d, 8)
            for i in range(2):
                r_snd[h, d, i] = sums(ptr3, peer * 2 + i)
            part_three(h, d).start()
        for i in range(2):
            own3[h, i] = own3[h, i] + sums(ptr3, row * 2 + i)

    def final_three(h):
        for d in range(1, 8):
            part_three(h, d).wait_recv()
        for i in range(2):
            total = own3[h, i]
            for d in range(1, 8):
                total = total + r_got[h, d, i]
            out3[h, i] = total.astype(BF16)
        pltpu.make_async_copy(out3.at[h], parts_hbm.at[h, pl.ds(40, 2)], o_sem.at[h, 2]).start()

    A, B = 0, 1
    inject_one(0, 4)
    load_t1.wait()
    products(A, 0, 5)
    products(A, 5, 10)
    products(A, 10, 14)
    products(A, 14, 16)
    sum_one(A)
    products(B, 0, 3)
    join(A)
    final_one(A)
    products(B, 3, 9)
    products(B, 9, 14)
    products(B, 14, 16)
    sum_one(B)
    pass_on(A)
    join(B)
    load_t2.wait()
    arrived(A)
    level_two(A)
    final_one(B)
    pass_on(B)
    final_two(A)
    arrived(B)
    load_t3.wait()
    level_two(B)
    level_three(A)
    final_two(B)
    level_three(B)
    final_three(A)
    final_three(B)

    for copy in asks:
        copy.wait_send()
    for h in range(2):
        for i in range(15):
            reply(h, i).wait_send()
            part_two(h, i).wait_send()
            spread_two(h, i).wait_send()
        for zt in range(4):
            to_partner(h, zt).wait_send()
        for i, zt in enumerate(zs + [z]):
            spread_chip(h, zt, i).wait_send()
        for i in range(3):
            along_z(h, i).wait_send()
            spread_z(h, i).wait_send()
        for d in range(1, 8):
            part_three(h, d).wait_send()
        pltpu.make_async_copy(piece(h, row), parts_hbm.at[h, pl.ds(0, 32)], o_sem.at[h, 0]).wait()
        pltpu.make_async_copy(
            g2[h].at[pl.ds(col * 8, 8)], parts_hbm.at[h, pl.ds(32, 8)], o_sem.at[h, 1]
        ).wait()
        pltpu.make_async_copy(out3.at[h], parts_hbm.at[h, pl.ds(40, 2)], o_sem.at[h, 2]).wait()


def on_device(
    fine, tiles1, ptr1, cols1, pts1, tiles2, ptr2, cols2, pts2, tiles3, ptr3, cols3, pts3
):
    n1 = tiles1.shape[0]
    hbm = pl.BlockSpec(memory_space=pl.ANY)
    vmem = pl.BlockSpec(memory_space=pltpu.VMEM)
    smem = pl.BlockSpec(memory_space=pltpu.SMEM)
    dma = pltpu.SemaphoreType.DMA
    vm = pltpu.VMEM
    ask, slot, tgt = pl.pallas_call(
        plan,
        out_shape=[
            jax.ShapeDtypeStruct((16, 1, E), I32),
            jax.ShapeDtypeStruct((16, 1, E), I32),
            jax.ShapeDtypeStruct((1, n1), I32),
        ],
        in_specs=[smem, vmem],
        out_specs=[vmem] * 3,
        name="plan",
    )(ptr1, cols1.reshape(1, n1))
    scratch = [
        vm(fine.shape, BF16), vm((2, 128, H, E), BF16), vm(tiles1.shape, BF16), vm(tiles2.shape, BF16), vm(tiles3.shape, BF16),
        pltpu.SMEM((16, 1, E), I32),
        vm((2, 15, 32, H, E), BF16), vm((2, 16, 32, H, E), BF16), vm((n1, H, E), F32), vm((n1 + 1, H, E), F32),
        vm((2, 4, 32, H, E), BF16), vm((2, 4, 32, H, E), BF16), vm((2, 4, 32, H, E), F32),
        vm((2, 3, 32, H, E), BF16), vm((2, 3, 32, H, E), BF16), vm((2, 32, H, E), F32), vm((256, H, E), BF16), vm((256, H, E), BF16),
        vm((2, 15, 8, H, E), BF16), vm((2, 15, 8, H, E), BF16), vm((2, 8, H, E), F32), vm((2, 8, H, E), F32), vm((128, H, E), BF16), vm((128, H, E), BF16),
        vm((2, 8, 2, H, E), F32), vm((2, 8, 2, H, E), F32), vm((2, 2, H, E), F32), vm((2, 2, H, E), BF16),
        dma((1,)), dma((3,)), dma((1,)),
        dma((15,)), dma((15,)), dma((2, 15)), dma((2, 15)), dma((2, 4)), dma((2, 4)), dma((2, 3)), dma((2, 3)), dma((2, 7)), dma((2, 8)),
        dma((2, 15)), dma((2, 15)), dma((2, 15)), dma((2, 15)), dma((2, 8)), dma((2, 8)), dma((2, 3)),
    ]
    parts = pl.pallas_call(
        kernel,
        out_shape=jax.ShapeDtypeStruct((2, 42, H, E), BF16),
        in_specs=[vmem] * 4 + [smem] * 7 + [hbm] * 4,
        out_specs=hbm,
        scratch_shapes=scratch,
        compiler_params=pltpu.CompilerParams(
            collective_id=0, has_side_effects=True, vmem_limit_bytes=58 << 20
        ),
        name="restrict",
    )(
        ask, pts1.reshape(-1, E), pts2.reshape(-1, E), pts3.reshape(-1, E),
        tgt, slot, ptr1, cols2, ptr2, cols3, ptr3, fine, tiles1, tiles2, tiles3,
    )
    return pl.pallas_call(
        emit,
        out_shape=tuple(
            jax.ShapeDtypeStruct((V, points.shape[0]), BF16) for points in (pts1, pts2, pts3)
        ),
        in_specs=[vmem],
        out_specs=(vmem,) * 3,
        name="emit",
    )(parts)


def solution(mesh):
    placed = (
        P(None, ("row", "col")),
        P(("row", "col"), None, None),
        P(("row", "col")),
        P(("row", "col")),
        P(("col", "row")),
        P(("row", "col"), None, None),
        P(("row", "col")),
        P(("row", "col")),
        P(("row", "col")),
        P(("row", "col"), None, None),
        P(("row", "col")),
        P(("row", "col")),
        P(("col", "row")),
    )
    return jax.shard_map(
        on_device,
        mesh=mesh,
        in_specs=placed,
        out_specs=(P(None, ("col", "row")), P(None, ("row", "col")), P(None, ("col", "row"))),
        check_vma=False,
    )
```
